32 devices in a mesh: rep: 2 (over z, core), dp: 16 (over x, y).
Axes of the slice: x: 4, y: 4, z: 1, core: 2. Of those that a mesh axis runs over, the one named last changes fastest.
The devices are a block of a 4x4x8 slice.
Arguments:
- x: bfloat16 [32, 4096, 896], P(('rep', 'dp')), parts along dimension 0
- dy: bfloat16 [32, 4096, 896], P(('rep', 'dp')), parts along dimension 0
- w_gate: bfloat16 [2, 896, 2560], P(None, 'dp')
- w_up: bfloat16 [2, 896, 2560], P(None, 'dp')
- w_down: bfloat16 [2, 2560, 896], P(None, 'dp')
- m_w_gate: float32 [2, 896, 2560], P(None, 'dp')
- m_w_up: float32 [2, 896, 2560], P(None, 'dp')
- m_w_down: float32 [2, 2560, 896], P(None, 'dp')
- v_w_gate: float32 [2, 896, 2560], P(None, 'dp')
- v_w_up: float32 [2, 896, 2560], P(None, 'dp')
- v_w_down: float32 [2, 2560, 896], P(None, 'dp')
Outputs:
- output 1: bfloat16 [4, 896, 2560], P('rep', 'dp'), parts along dimension 0
- output 2: bfloat16 [4, 896, 2560], P('rep', 'dp'), parts along dimension 0
- output 3: bfloat16 [4, 2560, 896], P('rep', 'dp'), parts along dimension 0
- output 4: float32 [4, 896, 2560], P('rep', 'dp'), parts along dimension 0
- output 5: float32 [4, 896, 2560], P('rep', 'dp'), parts along dimension 0
- output 6: float32 [4, 2560, 896], P('rep', 'dp'), parts along dimension 0
- output 7: float32 [4, 896, 2560], P('rep', 'dp'), parts along dimension 0
- output 8: float32 [4, 896, 2560], P('rep', 'dp'), parts along dimension 0
- output 9: float32 [4, 2560, 896], P('rep', 'dp'), parts along dimension 0
There are 2 independent parts. The reference program is written for one: setup_inputs(seed, part) draws one part's arguments, and reference() takes and returns one part's arrays. A program takes and returns all parts, laid end to end along the dimension named above; an argument that names none is the same for every part.
All inputs are finite; a program needn't handle non-finite values.
Results may differ from the reference program's by a relative error of at most 0.022.
Values are sent between devices in bfloat16 or wider.
A program may use at most 768 MiB of HBM per device.

```python
import jax
import jax.numpy as jnp
from jax import lax

SEQUENCES = 16
TOKENS = 4096
D = 896
FF = 2560
LAYERS = 2
NAMES = ("w_gate", "w_up", "w_down")
SHAPES = {"w_gate": (LAYERS, D, FF), "w_up": (LAYERS, D, FF), "w_down": (LAYERS, FF, D)}


def bump(key, n, height):
    away = (jnp.arange(n, dtype=jnp.int32) - jax.random.randint(key, (), 0, n, jnp.int32)) % n
    return jnp.where(away < n // 8, height, 1.0)


def together(key, own, strength):
    shared = jax.random.normal(key, own.shape[1:], jnp.float32)
    return (own + strength * shared) * lax.rsqrt(1 + strength * strength)


def setup_inputs(seed: int = 0, part: int = 0) -> dict:
    kx, kdy, ka, kb, kz, kf, kh, kl, *keys = jax.random.split(jax.random.key(seed), 8 + 3 * len(NAMES))
    kx, kdy, ka, kb = (jax.random.fold_in(k, part) for k in (kx, kdy, ka, kb))
    kw, km, kv = (keys[i::3] for i in range(3))
    shape = (SEQUENCES, TOKENS, D)
    much_x, much_dy = jax.random.uniform(kz, (2,), jnp.float32, 0.0, 1.0)
    loud = 2.0 ** jax.random.uniform(jax.random.fold_in(kz, 1), (), jnp.float32, -1.0, 2.0)
    layers = 2.0 ** jax.random.uniform(kl, (LAYERS, 1, 1), jnp.float32, -1.0, 1.0)
    x = together(ka, jax.random.normal(kx, shape, jnp.float32), much_x) * bump(kf, D, 4.0)
    dy = together(kb, jax.random.normal(kdy, shape, jnp.float32), much_dy)
    drawn = {"x": x.astype(jnp.bfloat16), "dy": (loud * dy * (SEQUENCES * TOKENS) ** -0.5).astype(jnp.bfloat16)}
    for key, name in zip(kw, NAMES, strict=True):
        w = jax.random.normal(key, SHAPES[name], jnp.float32) * SHAPES[name][1] ** -0.5
        drawn[name] = (w * {"w_gate": 1.0, "w_up": bump(kh, FF, 4.0), "w_down": layers}[name]).astype(jnp.bfloat16)
    for key, name in zip(km, NAMES, strict=True):
        drawn[f"m_{name}"] = 0.1 * jax.random.normal(key, SHAPES[name], jnp.float32)
    for key, name in zip(kv, NAMES, strict=True):
        drawn[f"v_{name}"] = jax.random.uniform(key, SHAPES[name], jnp.float32, 0.005, 0.015)
    return drawn


def matmul(a, w):
    return jnp.dot(a, w, preferred_element_type=jnp.float32).astype(jnp.bfloat16)


def normed(h):
    wide = h.astype(jnp.float32)
    scale = lax.rsqrt(jnp.mean(wide**2, -1, keepdims=True) + 1e-6)
    return (wide * scale).astype(jnp.bfloat16)


def layer(h, w):
    a = normed(h)
    gate = jnp.dot(a, w["w_gate"], preferred_element_type=jnp.float32)
    up = jnp.dot(a, w["w_up"], preferred_element_type=jnp.float32)
    return h + matmul((jax.nn.silu(gate) * up).astype(jnp.bfloat16), w["w_down"])


def adamw(w, m, v, g):
    m = 0.9 * m + 0.1 * g
    v = 0.95 * v + 0.05 * g * g
    step = m * lax.rsqrt(v + 1e-8) + 0.1 * w
    return (w - 0.02 * step).astype(jnp.bfloat16), m, v


def clipped(gradients, sum_of_squares, count):
    factor = jnp.minimum(1.0, 0.5 * lax.rsqrt(sum_of_squares / count + 1e-30))
    return [g * factor for g in gradients]


def stack(weights, h):
    return lax.scan(lambda h, w: (layer(h, w), None), h, weights)[0]


def reference(x, dy, w_gate, w_up, w_down, m_w_gate, m_w_up, m_w_down, v_w_gate, v_w_up, v_w_down):
    weights = dict(zip(NAMES, (w_gate, w_up, w_down), strict=True))

    def take(so_far, sequence):
        h, by_y = sequence
        _, back = jax.vjp(lambda w: stack(w, h), weights)
        return jax.tree.map(lambda total, term: total + term.astype(jnp.float32), so_far, back(by_y)[0]), None

    none_yet = {name: jnp.zeros(w.shape, jnp.float32) for name, w in weights.items()}
    by_weights, _ = lax.scan(take, none_yet, (x, dy))
    gradients = [by_weights[name].astype(jnp.bfloat16).astype(jnp.float32) for name in NAMES]
    gradients = clipped(gradients, sum(jnp.sum(g * g) for g in gradients), sum(g.size for g in gradients))
    new = [
        adamw(w.astype(jnp.float32), m, v, g)
        for w, m, v, g in zip((w_gate, w_up, w_down), (m_w_gate, m_w_up, m_w_down), (v_w_gate, v_w_up, v_w_down), gradients, strict=True)
    ]
    return tuple(one[which] for which in range(3) for one in new)
```

```python
import math

import jax
import jax.numpy as jnp
from jax import lax
from jax.experimental import pallas as pl
from jax.experimental.pallas import tpu as pltpu
from jax.sharding import PartitionSpec as P

MESH = pl.DeviceIdType.MESH
F32, BF16 = jnp.float32, jnp.bfloat16
ANY = pl.BlockSpec(memory_space=pl.ANY)
DMA = pltpu.SemaphoreType.DMA
CHUNK = 512
ROWS, TOKENS = 256, 512


class Spot:
    def __init__(self, side):
        self.side = side
        rep, self.dp = lax.axis_index("rep"), lax.axis_index("dp")
        c = self.c = lax.rem(rep, 2)
        hi, lo = self.dp // side, lax.rem(self.dp, side)
        self.f, self.s = hi * c + lo * (1 - c), lo * c + hi * (1 - c)
        self.partner = rep + 1 - 2 * c

    def at(self, f, s):
        f, s, c, side = lax.rem(f, self.side), lax.rem(s, self.side), self.c, self.side
        return f * (1 - c + side * c) + s * (side * (1 - c) + c)

    def near(self, df, ds):
        return self.at(self.f + df, self.s + ds)


def greet(places, partner=None):
    barrier = pltpu.get_barrier_semaphore()
    for place in places:
        pl.semaphore_signal(barrier, inc=1, device_id={"dp": place}, device_id_type=MESH)
    if partner is not None:
        pl.semaphore_signal(barrier, inc=1, device_id={"rep": partner}, device_id_type=MESH)
    pl.semaphore_wait(barrier, len(places) + (partner is not None))


def send(src, dst, out, came, **to):
    pltpu.make_async_remote_copy(src_ref=src, dst_ref=dst, send_sem=out, recv_sem=came, device_id=to, device_id_type=MESH).start()


def bring(src, dst, sem):
    pltpu.make_async_copy(src, dst, sem).start()


def await_bytes(like, sem):
    pltpu.make_async_copy(like, like, sem).wait()


def call(body, n, grid, in_specs, out_specs, out_shape, scratch, number, cost):
    def kernel(*refs):
        body(refs[:n], refs[n : n + len(out_shape)], refs[n + len(out_shape) :])

    return pl.pallas_call(
        kernel,
        grid=grid,
        in_specs=in_specs,
        out_specs=out_specs,
        out_shape=out_shape,
        scratch_shapes=scratch,
        compiler_params=pltpu.CompilerParams(
            dimension_semantics=("arbitrary",) * len(grid),
            vmem_limit_bytes=66_000_000,
            **({} if number is None else {"collective_id": number, "has_side_effects": True}),
        ),
        cost_estimate=pl.CostEstimate(flops=cost, bytes_accessed=cost // 400, transcendentals=0),
    )


def gather_scratch(rows, columns):
    return [pltpu.VMEM((rows, columns), BF16), DMA((2,)), DMA((2,)), DMA((6,))]


def gather_stages(spot, shards, layer, full, scratch):
    held, local, out, came = scratch
    rows, columns = held.shape
    by_columns = columns > 1024
    side = spot.side
    me, c = spot.dp, spot.c

    def part(ref, lead, cuts, number):
        if by_columns:
            width = columns // cuts
            return ref.at[lead, :, pl.ds(pl.multiple_of(number * width, 128), width)]
        height = rows // cuts
        return ref.at[lead, pl.ds(pl.multiple_of(number * height, 8), height), :]

    def unit(p):
        return part(full, p, 2, c)

    def quarter(p, q):
        return part(full, p, 4, 2 * c + q)

    def units(n):
        return part(full, pl.ds(0, n), 2, 0)

    def quarters(n):
        return part(full, pl.ds(0, n), 4, 0)

    mine = part(shards, layer, 2, c)

    def start():
        for df in (1, side - 1, 2):
            send(mine, unit(me), out.at[0], came.at[0], dp=spot.near(df, 0))
        fill = pltpu.make_async_copy(shards.at[layer], held, local.at[0])
        fill.start()
        fill.wait()
        bring(held, full.at[me], local.at[1])

    def across():
        await_bytes(units(side - 1), came.at[0])
        for df in range(side):
            p = spot.near(df, 0)
            source = unit(p) if df else mine
            send(source, unit(p), out.at[0], came.at[1], dp=spot.near(0, 1))
            send(source, unit(p), out.at[0], came.at[2], dp=spot.near(0, side - 1))
            if df:
                send(unit(p), unit(p), out.at[1], came.at[5], rep=spot.partner)

    def onward():
        await_bytes(units(side), came.at[1])
        await_bytes(units(side), came.at[2])
        for df in range(side):
            p, q = spot.near(df, side - 1), spot.near(df, 1)
            send(quarter(p, 0), quarter(p, 0), out.at[0], came.at[3], dp=spot.near(0, 1))
            send(quarter(q, 1), quarter(q, 1), out.at[0], came.at[4], dp=spot.near(0, side - 1))
        for df in range(side):
            for ds in (1, side - 1):
                p = spot.near(df, ds)
                send(unit(p), unit(p), out.at[1], came.at[5], rep=spot.partner)

    def last():
        await_bytes(quarters(side), came.at[3])
        await_bytes(quarters(side), came.at[4])
        for df in range(side):
            p = spot.near(df, 2)
            send(unit(p), unit(p), out.at[1], came.at[5], rep=spot.partner)

    def finish():
        n = side * side - 1
        await_bytes(units(n), came.at[5])
        await_bytes(units(n), out.at[0])
        await_bytes(units(n), out.at[1])
        await_bytes(held, local.at[1])

    return start, across, onward, last, finish


def greet_for_gather(spot):
    greet([spot.near(df, ds) for df, ds in ((1, 0), (spot.side - 1, 0), (2, 0), (0, 1), (0, spot.side - 1))], spot.partner)


def half_shape(rows, columns):
    return (rows, columns // 2) if columns > 1024 else (rows // 2, columns)


def half_of(ref, p, h):
    rows, columns = ref.shape[1:]
    if columns > 1024:
        return ref.at[p, :, pl.ds(h * (columns // 2), columns // 2)]
    return ref.at[p, pl.ds(h * (rows // 2), rows // 2), :]


def ring_scratch(n, half):
    return [pltpu.VMEM((n, *half), BF16)] * 10 + [DMA((4,)), DMA((6,)), DMA((6,))]


def ring_stages(source, place, side, plus, minus, scratch, own, done):
    across_a, across_b, next_a, prev_b, here_a, here_b, up_a, up_b, down_a, down_b, local, out, came = scratch
    n = across_a.shape[0]
    following, before, opposite = (lax.rem(place + d, side) for d in (1, side - 1, 2))

    def start():
        for k in range(n):
            send(source(opposite, k, 0), across_a.at[k], out.at[0], came.at[0], dp=plus)
            send(source(opposite, k, 1), across_b.at[k], out.at[1], came.at[1], dp=minus)
        for k in range(n):
            send(source(following, k, 1), up_b.at[k], out.at[2], came.at[2], dp=plus)
            send(source(before, k, 0), down_a.at[k], out.at[3], came.at[3], dp=minus)
        for k in range(n):
            bring(source(following, k, 0), next_a.at[k], local.at[0])
            bring(source(before, k, 1), prev_b.at[k], local.at[1])
            if own is None:
                bring(source(place, k, 0), here_a.at[k], local.at[2])
                bring(source(place, k, 1), here_b.at[k], local.at[3])

    def add():
        for which, (mine, theirs, landing, to) in enumerate(((next_a, across_a, up_a, plus), (prev_b, across_b, down_b, minus))):
            await_bytes(mine, local.at[which])
            await_bytes(theirs, came.at[which])
            for k in range(n):
                mine[k] = (mine[k].astype(F32) + theirs[k].astype(F32)).astype(BF16)
            for k in range(n):
                send(mine.at[k], landing.at[k], out.at[4 + which], came.at[4 + which], dp=to)

    def finish():
        if own is None:
            await_bytes(here_a, local.at[2])
            await_bytes(here_b, local.at[3])
        for number, ref in zip((2, 3, 4, 5), (up_b, down_a, up_a, down_b), strict=True):
            await_bytes(ref, came.at[number])
        for k in range(n):
            for h, here, up, down in ((0, here_a, up_a, down_a), (1, here_b, up_b, down_b)):
                term = here[k].astype(F32) if own is None else own[h]
                done(k, h, term + up[k].astype(F32) + down[k].astype(F32))
        for number in range(6):
            await_bytes(across_a, out.at[number])

    return start, add, finish


def first_ring(spot, blocks, scratch, partial, kept):
    def done(k, h, total):
        partial[k, h] = total.astype(BF16)

        @pl.when(spot.s == k)
        def _():
            kept[h] = total

    def source(j, k, h):
        return half_of(blocks, spot.at(j, k), h)

    return ring_stages(source, spot.f, spot.side, spot.near(1, 0), spot.near(spot.side - 1, 0), scratch, None, done)


def second_ring(spot, partial, kept, scratch, result):
    def done(k, h, total):
        result[h] = total.astype(BF16)

    def source(j, k, h):
        return partial.at[j, h]

    return ring_stages(source, spot.s, spot.side, spot.near(0, 1), spot.near(0, spot.side - 1), scratch, kept, done)


def dot(a, b):
    return jnp.dot(a, b, preferred_element_type=F32)


def dot_t(a, b):
    return lax.dot_general(a, b, (((1,), (1,)), ((), ())), preferred_element_type=F32)


def scale_of(wide):
    return lax.rsqrt(jnp.mean(wide * wide, -1, keepdims=True) + 1e-6)


def gated_back(gate, up, by_act):
    s = jax.nn.sigmoid(gate)
    silu = gate * s
    return silu, (by_act * up * (s + silu * (1 - s))).astype(BF16), (by_act * silu).astype(BF16)


def cuts(n):
    return [pl.ds(at, CHUNK) for at in range(0, n, CHUNK)]


def put_blocks(out, total):
    blocks, rows, _ = out.shape
    for p in range(blocks):
        out[p] = total[pl.ds(p * rows, rows), :].astype(BF16)


def whole(shape):
    return pl.BlockSpec(shape, lambda i: (0,) * len(shape), pipeline_mode=pl.Buffered(1))


def fixed(shape):
    return pl.BlockSpec(shape, lambda i: (0,) * len(shape))


def tile(rows, columns):
    return pl.BlockSpec((rows, columns), lambda i: (i, 0))


def tile_of_one(rows, columns):
    return pl.BlockSpec((None, rows, columns), lambda i: (0, i, 0))


def struct(shape, dtype=BF16):
    return jax.ShapeDtypeStruct(shape, dtype)


def solution(mesh):
    group = mesh.shape["dp"]
    side = math.isqrt(group)

    def gather_only(shards, layer):
        shapes = [w.shape[1:] for w in shards]

        def body(ins, outs, scratch):
            spot = Spot(side)
            greet_for_gather(spot)
            stages = [gather_stages(spot, ins[i], layer, outs[i], scratch[4 * i : 4 * i + 4]) for i in range(3)]
            for stage in zip(*stages, strict=True):
                for run in stage:
                    run()

        scratch = [one for shape in shapes for one in gather_scratch(*shape)]
        outs = [struct((group, *shape)) for shape in shapes]
        return call(body, 3, (), [ANY] * 3, [ANY] * 3, outs, scratch, 0, 1000)(*shards)

    def forward(x, weights, shards, layer):
        _, tokens, d = x.shape
        ff = weights[0].shape[1]
        steps = tokens // ROWS
        shapes = [w.shape[1:] for w in shards]

        def body(ins, outs, scratch):
            x, w_gate, w_up, w_down, *shards = ins
            a_out, gate_out, up_out, act_out, h_out, *full = outs
            i = pl.program_id(0)
            spot = Spot(side)
            stages = [gather_stages(spot, shards[j], layer, full[j], scratch[4 * j : 4 * j + 4]) for j in range(3)]
            for number, when in enumerate((0, 3, 8, 11)):

                @pl.when(i == when)
                def _():
                    if number == 0:
                        greet_for_gather(spot)
                    for one in stages:
                        one[number]()

            wide = x[...].astype(F32)
            a = (wide * scale_of(wide)).astype(BF16)
            a_out[...] = a
            for cut in cuts(ff):
                gate, up = dot(a, w_gate[:, cut]), dot(a, w_up[:, cut])
                gate_out[:, cut], up_out[:, cut] = gate, up
                act_out[:, cut] = (gate * jax.nn.sigmoid(gate) * up).astype(BF16)
            h_out[...] = (wide + dot(act_out[...], w_down[...]).astype(BF16).astype(F32)).astype(BF16)

            @pl.when(i == steps - 1)
            def _():
                for one in stages:
                    one[4]()

        scratch = [one for shape in shapes for one in gather_scratch(*shape)]
        wide = [struct((tokens, ff), F32)] * 2
        outs = [struct((tokens, d)), *wide, struct((tokens, ff)), struct((tokens, d))] + [struct((group, *s)) for s in shapes]
        out_specs = [tile(ROWS, d)] + [tile(ROWS, ff)] * 3 + [tile(ROWS, d)] + [ANY] * 3
        in_specs = [tile_of_one(ROWS, d)] + [whole(w.shape) for w in weights] + [ANY] * 3
        return call(body, 7, (steps,), in_specs, out_specs, outs, scratch, 1, 6 * tokens * d * ff)(x, *weights, *shards)

    def last_layer(h, dy, weights):
        tokens, d = h.shape
        ff = weights[0].shape[1]
        steps = tokens // ROWS
        rows = ff // group

        def body(ins, outs, scratch):
            h, dy, w_gate, w_up, w_down = ins
            a_out, by_gate, by_up, by_h, by_down = outs
            total, act = scratch
            i = pl.program_id(0)

            @pl.when(i == 0)
            def _():
                total[...] = jnp.zeros_like(total)

            wide = h[...].astype(F32)
            scale = scale_of(wide)
            a = (wide * scale).astype(BF16)
            a_out[...] = a
            by_y = dy[...]
            for cut in cuts(ff):
                gate, up = dot(a, w_gate[:, cut]), dot(a, w_up[:, cut])
                by_act = dot_t(by_y, w_down[cut, :]).astype(BF16).astype(F32)
                silu, by_gate[:, cut], by_up[:, cut] = gated_back(gate, up, by_act)
                act[:, cut] = (silu * up).astype(BF16)
            by_a = dot_t(by_gate[...], w_gate[...]).astype(BF16).astype(F32) + dot_t(by_up[...], w_up[...]).astype(BF16).astype(F32)
            by_a = by_a.astype(BF16).astype(F32)
            inner = jnp.sum(by_a * wide, -1, keepdims=True) * (scale * scale * scale) * (1 / d)
            by_x = (by_a * scale - wide * inner).astype(BF16)
            by_h[...] = (by_y.astype(F32) + by_x.astype(F32)).astype(BF16)
            for cut in cuts(ff):
                total[cut, :] += dot(act[:, cut].T, by_y)

            @pl.when(i == steps - 1)
            def _():
                put_blocks(by_down, total)

        outs = [struct((tokens, d)), struct((tokens, ff)), struct((tokens, ff)), struct((tokens, d)), struct((group, rows, d))]
        out_specs = [tile(ROWS, d), tile(ROWS, ff), tile(ROWS, ff), tile(ROWS, d), fixed((group, rows, d))]
        in_specs = [tile(ROWS, d), tile_of_one(ROWS, d)] + [whole(w.shape) for w in weights]
        scratch = [pltpu.VMEM((ff, d), F32), pltpu.VMEM((ROWS, ff), BF16)]
        return call(body, 5, (steps,), in_specs, out_specs, outs, scratch, None, 12 * tokens * d * ff)(h, dy, *weights)

    def hidden(compute, n_in, n_out, steps, number, first, second):
        more_in, more_specs, more_out, more_out_specs, more_scratch = [], [], [], [], []
        if first is not None:
            half = half_shape(*first.shape[1:])
            more_in += [first]
            more_specs += [ANY]
            more_out += [struct((side, 2, *half)), struct((2, *half), F32)]
            more_out_specs += [fixed((side, 2, *half)), fixed((2, *half))]
            more_scratch += ring_scratch(side, half)
        if second is not None:
            partial, kept = second
            half = partial.shape[2:]
            more_in += [partial, kept]
            more_specs += [ANY, whole(kept.shape)]
            more_out += [struct((2, *half))]
            more_out_specs += [fixed((2, *half))]
            more_scratch += ring_scratch(1, half)

        def body(ins, outs, scratch):
            i = pl.program_id(0)
            spot = Spot(side)
            own = len(scratch) - len(more_scratch)
            ins_left, outs_left, scratch_left = list(ins[n_in:]), list(outs[n_out:]), list(scratch[own:])
            plan = []
            if first is not None:
                stages = first_ring(spot, ins_left.pop(0), scratch_left[:13], outs_left.pop(0), outs_left.pop(0))
                del scratch_left[:13]
                plan += list(zip((0, (5 * steps) // 8, None), stages, strict=True))
            if second is not None:
                stages = second_ring(spot, ins_left.pop(0), ins_left.pop(0), scratch_left, outs_left.pop(0))
                plan += list(zip((0, (3 * steps) // 8, (6 * steps) // 8), stages, strict=True))

            @pl.when(i == 0)
            def _():
                greet([spot.near(*way) for way in ((1, 0), (side - 1, 0), (0, 1), (0, side - 1))])

            for when, run in plan:
                if when is not None:
                    pl.when(i == when)(run)
            compute(i, ins[:n_in], outs[:n_out], scratch[:own])
            for when, run in plan:
                if when is None:
                    pl.when(i == steps - 1)(run)

        return body, more_in, more_specs, more_out, more_out_specs, more_scratch

    def weight_gradient(a, by, number, first, second):
        tokens, m = a.shape
        n = by.shape[1]
        steps = tokens // TOKENS
        rows = m // group

        def compute(i, ins, outs, scratch):
            a, by = ins
            (total,) = scratch

            @pl.when(i == 0)
            def _():
                total[...] = jnp.zeros_like(total)

            if n > m:
                left = a[...].T
                for cut in cuts(n):
                    total[:, cut] += dot(left, by[:, cut])
            else:
                right = by[...]
                for cut in cuts(m):
                    total[cut, :] += dot(a[:, cut].T, right)

            @pl.when(i == steps - 1)
            def _():
                put_blocks(outs[0], total)

        body, ins, specs, outs, out_specs, scratch = hidden(compute, 2, 1, steps, number, first, second)
        return call(
            body,
            2 + len(ins),
            (steps,),
            [tile(TOKENS, m), tile(TOKENS, n), *specs],
            [fixed((group, rows, n)), *out_specs],
            [struct((group, rows, n)), *outs],
            [pltpu.VMEM((m, n), F32), *scratch],
            number,
            2 * tokens * m * n,
        )(a, by, *ins)

    def gate_gradient(by_h, gate, up, a, w_down, number, first, second):
        tokens, d = a.shape
        ff = gate.shape[1]
        steps = tokens // ROWS
        rows = d // group

        def compute(i, ins, outs, scratch):
            by_h, gate, up, a, w_down = ins
            by_up, by_w = outs
            (total,) = scratch

            @pl.when(i == 0)
            def _():
                total[...] = jnp.zeros_like(total)

            by_y, left = by_h[...], a[...].T
            for cut in cuts(ff):
                by_act = dot_t(by_y, w_down[cut, :]).astype(BF16).astype(F32)
                _, by_gate, by_up[:, cut] = gated_back(gate[:, cut], up[:, cut], by_act)
                total[:, cut] += dot(left, by_gate)

            @pl.when(i == steps - 1)
            def _():
                put_blocks(by_w, total)

        body, ins, specs, outs, out_specs, scratch = hidden(compute, 5, 2, steps, number, first, second)
        return call(
            body,
            5 + len(ins),
            (steps,),
            [tile(ROWS, d), tile(ROWS, ff), tile(ROWS, ff), tile(ROWS, d), whole(w_down.shape), *specs],
            [tile(ROWS, ff), fixed((group, rows, ff)), *out_specs],
            [struct((tokens, ff)), struct((group, rows, ff)), *outs],
            [pltpu.VMEM((d, ff), F32), *scratch],
            number,
            4 * tokens * d * ff,
        )(by_h, gate, up, a, w_down, *ins)

    def closing(first, second, ready, number):
        half = half_shape(*first.shape[1:])
        n = len(ready)

        def body(ins, outs, scratch):
            blocks, partial, kept, *ready = ins
            late, last, squares = outs
            spot = Spot(side)
            greet([spot.near(*way) for way in ((1, 0), (side - 1, 0), (2, 0), (0, 1), (0, side - 1), (0, 2))])
            ring_1, ring_2, ring_3 = scratch[:13], scratch[13:26], scratch[26:39]
            partial_2, kept_2, sums, out, came = scratch[39:]
            one = first_ring(spot, blocks, ring_1, partial_2, kept_2)
            two = second_ring(spot, partial, kept, ring_2, late)
            three = second_ring(spot, partial_2, kept_2, ring_3, last)
            one[0]()
            two[0]()
            two[1]()
            one[1]()
            two[2]()
            total = jnp.zeros((1, 1), F32)
            for g in [*ready, late]:
                for h in range(2):
                    wide = g[h].astype(F32)
                    total += jnp.sum(wide * wide, keepdims=True)
            one[2]()
            three[0]()
            three[1]()
            three[2]()
            for h in range(2):
                wide = last[h].astype(F32)
                total += jnp.sum(wide * wide, keepdims=True)
            for axis in range(2):
                sums[axis, 0] = jnp.broadcast_to(total, sums.shape[2:])
                for d in range(1, side):
                    to = spot.near(d, 0) if axis == 0 else spot.near(0, d)
                    send(sums.at[axis, 0], sums.at[axis, d], out.at[axis, d - 1], came.at[axis, d - 1], dp=to)
                for d in range(1, side):
                    await_bytes(sums.at[axis, 0], came.at[axis, d - 1])
                for d in range(1, side):
                    total = total + sums[axis, d, 0:1, 0:1]
                for d in range(1, side):
                    await_bytes(sums.at[axis, 0], out.at[axis, d - 1])
            squares[...] = jnp.broadcast_to(total, squares.shape)

        vmem = pl.BlockSpec(memory_space=pltpu.VMEM)
        partial, kept = second
        scratch = ring_scratch(side, half) + ring_scratch(1, half) * 2
        scratch += [pltpu.VMEM((side, 2, *half), BF16), pltpu.VMEM((2, *half), F32), pltpu.VMEM((2, side, 8, 128), F32)]
        scratch += [DMA((2, side - 1)), DMA((2, side - 1))]
        outs = [struct((2, *half)), struct((2, *half)), struct((8, 128), F32)]
        return call(body, 3 + n, (), [ANY, ANY, vmem] + [vmem] * n, [vmem] * 3, outs, scratch, number, 1000)(first, partial, kept, *ready)

    def adamw(w, m, v, g):
        m = 0.9 * m + 0.1 * g
        v = 0.95 * v + 0.05 * g * g
        step = m * lax.rsqrt(v + 1e-8) + 0.1 * w
        return (w - 0.02 * step).astype(BF16), m, v

    def joined(g, shape):
        return jnp.concatenate([g[0], g[1]], 1 if shape[1] > 1024 else 0)

    def step(x, dy, *arrays):
        weights, m, v = (arrays[i : i + 3] for i in (0, 3, 6))
        flat = lambda full: [w.reshape(-1, w.shape[2]) for w in full]
        w_0 = flat(gather_only(weights, 0))
        a_0, gate, up, act, h, *full = forward(x, w_0, weights, 1)
        a_1, by_gate, by_up, by_h, down_1 = last_layer(h, dy, flat(full))
        gate_1, *down_1 = weight_gradient(a_1, by_gate, 2, down_1, None)
        up_1, *gate_1, down_1 = weight_gradient(a_1, by_up, 3, gate_1, down_1)
        down_0, *up_1, gate_1 = weight_gradient(act, by_h, 4, up_1, gate_1)
        by_up, gate_0, *down_0, up_1 = gate_gradient(by_h, gate, up, a_0, w_0[2], 5, down_0, up_1)
        up_0, *gate_0, down_0 = weight_gradient(a_0, by_up, 6, gate_0, down_0)
        gate_0, up_0, squares = closing(up_0, gate_0, [down_1, gate_1, up_1, down_0], 7)
        count = group * sum(w.size for w in weights)
        factor = jnp.minimum(1.0, 0.5 * lax.rsqrt(squares[0, 0] / count + 1e-30))
        pairs = ((gate_0, gate_1), (up_0, up_1), (down_0, down_1))
        new = []
        for w, m_w, v_w, pair in zip(weights, m, v, pairs, strict=True):
            g = jnp.stack([joined(one, w.shape[1:]) for one in pair]).astype(F32) * factor
            new.append(adamw(w.astype(F32), m_w, v_w, g))
        return tuple(one[which] for which in range(3) for one in new)

    states, cut = P(("rep", "dp"), None, None), P(None, "dp", None)
    return jax.shard_map(
        step,
        mesh=mesh,
        in_specs=(states, states) + (cut,) * 9,
        out_specs=(P("rep", "dp", None),) * 9,
        check_vma=False,
    )
```

```python
import math

import jax
import jax.numpy as jnp
from jax import lax
from jax.experimental import pallas as pl
from jax.experimental.pallas import tpu as pltpu
from jax.sharding import PartitionSpec as P

MESH = pl.DeviceIdType.MESH
F32, BF16 = jnp.float32, jnp.bfloat16
ANY = pl.BlockSpec(memory_space=pl.ANY)
DMA = pltpu.SemaphoreType.DMA
CHUNK = 512
ROWS, TOKENS = 256, 512


class Spot:
    def __init__(self, side):
        self.side = side
        rep, self.dp = lax.axis_index("rep"), lax.axis_index("dp")
        c = self.c = lax.rem(rep, 2)
        hi, lo = self.dp // side, lax.rem(self.dp, side)
        self.f, self.s = hi * c + lo * (1 - c), lo * c + hi * (1 - c)
        self.partner = rep + 1 - 2 * c

    def at(self, f, s):
        f, s, c, side = lax.rem(f, self.side), lax.rem(s, self.side), self.c, self.side
        return f * (1 - c + side * c) + s * (side * (1 - c) + c)

    def near(self, df, ds):
        return self.at(self.f + df, self.s + ds)


def greet(places, partner=None):
    barrier = pltpu.get_barrier_semaphore()
    for place in places:
        pl.semaphore_signal(barrier, inc=1, device_id={"dp": place}, device_id_type=MESH)
    if partner is not None:
        pl.semaphore_signal(barrier, inc=1, device_id={"rep": partner}, device_id_type=MESH)
    pl.semaphore_wait(barrier, len(places) + (partner is not None))


def send(src, dst, out, came, **to):
    pltpu.make_async_remote_copy(src_ref=src, dst_ref=dst, send_sem=out, recv_sem=came, device_id=to, device_id_type=MESH).start()


def bring(src, dst, sem):
    pltpu.make_async_copy(src, dst, sem).start()


def await_bytes(like, sem):
    pltpu.make_async_copy(like, like, sem).wait()


def call(body, n, grid, in_specs, out_specs, out_shape, scratch, number, cost):
    def kernel(*refs):
        body(refs[:n], refs[n : n + len(out_shape)], refs[n + len(out_shape) :])

    return pl.pallas_call(
        kernel,
        grid=grid,
        in_specs=in_specs,
        out_specs=out_specs,
        out_shape=out_shape,
        scratch_shapes=scratch,
        compiler_params=pltpu.CompilerParams(
            dimension_semantics=("arbitrary",) * len(grid),
            vmem_limit_bytes=66_000_000,
            **({} if number is None else {"collective_id": number, "has_side_effects": True}),
        ),
        cost_estimate=pl.CostEstimate(flops=cost, bytes_accessed=cost // 400, transcendentals=0),
    )


def gather_scratch(rows, columns):
    return [pltpu.VMEM((rows, columns), BF16), DMA((2,)), DMA((2,)), DMA((9,))]


def gather_stages(spot, shards, layer, full, scratch):
    held, local, out, came = scratch
    rows, columns = held.shape
    by_columns = columns > 1024
    side = spot.side
    me, c = spot.dp, spot.c

    def part(ref, lead, cuts, number):
        if by_columns:
            width = columns // cuts
            return ref.at[lead, :, pl.ds(pl.multiple_of(number * width, 128), width)]
        height = rows // cuts
        return ref.at[lead, pl.ds(pl.multiple_of(number * height, 8), height), :]

    def unit(p):
        return part(full, p, 2, c)

    def quarter(p, q):
        return part(full, p, 4, 2 * c + q)

    def units(n):
        return part(full, pl.ds(0, n), 2, 0)

    def quarters(n):
        return part(full, pl.ds(0, n), 4, 0)

    mine = part(shards, layer, 2, c)

    def start():
        send(mine, unit(me), out.at[0], came.at[0], dp=spot.near(1, 0))
        send(mine, unit(me), out.at[0], came.at[6], dp=spot.near(side - 1, 0))
        fill = pltpu.make_async_copy(shards.at[layer], held, local.at[0])
        fill.start()
        fill.wait()
        bring(held, full.at[me], local.at[1])

    def relay():
        p, q = spot.near(side - 1, 0), spot.near(1, 0)
        await_bytes(unit(p), came.at[0])
        send(quarter(p, 0), quarter(p, 0), out.at[0], came.at[7], dp=spot.near(1, 0))
        await_bytes(unit(q), came.at[6])
        send(quarter(q, 1), quarter(q, 1), out.at[0], came.at[8], dp=spot.near(side - 1, 0))

    def across():
        await_bytes(quarter(me, 0), came.at[7])
        await_bytes(quarter(me, 1), came.at[8])
        for df in range(side):
            p = spot.near(df, 0)
            source = unit(p) if df else mine
            send(source, unit(p), out.at[0], came.at[1], dp=spot.near(0, 1))
            send(source, unit(p), out.at[0], came.at[2], dp=spot.near(0, side - 1))
            if df:
                send(unit(p), unit(p), out.at[1], came.at[5], rep=spot.partner)

    def onward():
        await_bytes(units(side), came.at[1])
        await_bytes(units(side), came.at[2])
        for df in range(side):
            p, q = spot.near(df, side - 1), spot.near(df, 1)
            send(quarter(p, 0), quarter(p, 0), out.at[0], came.at[3], dp=spot.near(0, 1))
            send(quarter(q, 1), quarter(q, 1), out.at[0], came.at[4], dp=spot.near(0, side - 1))
        for df in range(side):
            for ds in (1, side - 1):
                p = spot.near(df, ds)
                send(unit(p), unit(p), out.at[1], came.at[5], rep=spot.partner)

    def last():
        await_bytes(quarters(side), came.at[3])
        await_bytes(quarters(side), came.at[4])
        for df in range(side):
            p = spot.near(df, 2)
            send(unit(p), unit(p), out.at[1], came.at[5], rep=spot.partner)

    def finish():
        n = side * side - 1
        await_bytes(units(n), came.at[5])
        await_bytes(units(n), out.at[0])
        await_bytes(units(n), out.at[1])
        await_bytes(held, local.at[1])

    return start, relay, across, onward, last, finish


def greet_for_gather(spot):
    greet([spot.near(df, ds) for df, ds in ((1, 0), (spot.side - 1, 0), (0, 1), (0, spot.side - 1))], spot.partner)


def half_shape(rows, columns):
    return (rows, columns // 2) if columns > 1024 else (rows // 2, columns)


def half_of(ref, p, h):
    rows, columns = ref.shape[1:]
    if columns > 1024:
        return ref.at[p, :, pl.ds(h * (columns // 2), columns // 2)]
    return ref.at[p, pl.ds(h * (rows // 2), rows // 2), :]


def ring_scratch(n, half):
    return [pltpu.VMEM((n, *half), BF16)] * 10 + [DMA((4,)), DMA((6,)), DMA((6,))]


def ring_stages(source, place, side, plus, minus, scratch, own, done):
    across_a, across_b, next_a, prev_b, here_a, here_b, up_a, up_b, down_a, down_b, local, out, came = scratch
    n = across_a.shape[0]
    following, before, opposite = (lax.rem(place + d, side) for d in (1, side - 1, 2))

    def start():
        for k in range(n):
            send(source(opposite, k, 0), across_a.at[k], out.at[0], came.at[0], dp=plus)
            send(source(opposite, k, 1), across_b.at[k], out.at[1], came.at[1], dp=minus)
        for k in range(n):
            send(source(following, k, 1), up_b.at[k], out.at[2], came.at[2], dp=plus)
            send(source(before, k, 0), down_a.at[k], out.at[3], came.at[3], dp=minus)
        for k in range(n):
            bring(source(following, k, 0), next_a.at[k], local.at[0])
            bring(source(before, k, 1), prev_b.at[k], local.at[1])
            if own is None:
                bring(source(place, k, 0), here_a.at[k], local.at[2])
                bring(source(place, k, 1), here_b.at[k], local.at[3])

    def add():
        for which, (mine, theirs, landing, to) in enumerate(((next_a, across_a, up_a, plus), (prev_b, across_b, down_b, minus))):
            await_bytes(mine, local.at[which])
            await_bytes(theirs, came.at[which])
            for k in range(n):
                mine[k] = (mine[k].astype(F32) + theirs[k].astype(F32)).astype(BF16)
            for k in range(n):
                send(mine.at[k], landing.at[k], out.at[4 + which], came.at[4 + which], dp=to)

    def finish():
        if own is None:
            await_bytes(here_a, local.at[2])
            await_bytes(here_b, local.at[3])
        for number, ref in zip((2, 3, 4, 5), (up_b, down_a, up_a, down_b), strict=True):
            await_bytes(ref, came.at[number])
        for k in range(n):
            for h, here, up, down in ((0, here_a, up_a, down_a), (1, here_b, up_b, down_b)):
                term = here[k].astype(F32) if own is None else own[h]
                done(k, h, term + up[k].astype(F32) + down[k].astype(F32))
        for number in range(6):
            await_bytes(across_a, out.at[number])

    return start, add, finish


def first_ring(spot, blocks, scratch, partial, kept):
    def done(k, h, total):
        partial[k, h] = total.astype(BF16)

        @pl.when(spot.s == k)
        def _():
            kept[h] = total

    def source(j, k, h):
        return half_of(blocks, spot.at(j, k), h)

    return ring_stages(source, spot.f, spot.side, spot.near(1, 0), spot.near(spot.side - 1, 0), scratch, None, done)


def second_ring(spot, partial, kept, scratch, result):
    def done(k, h, total):
        result[h] = total.astype(BF16)

    def source(j, k, h):
        return partial.at[j, h]

    return ring_stages(source, spot.s, spot.side, spot.near(0, 1), spot.near(0, spot.side - 1), scratch, kept, done)


def dot(a, b):
    return jnp.dot(a, b, preferred_element_type=F32)


def dot_t(a, b):
    return lax.dot_general(a, b, (((1,), (1,)), ((), ())), preferred_element_type=F32)


def scale_of(wide):
    return lax.rsqrt(jnp.mean(wide * wide, -1, keepdims=True) + 1e-6)


def gated_back(gate, up, by_act):
    s = jax.nn.sigmoid(gate)
    silu = gate * s
    return silu, (by_act * up * (s + silu * (1 - s))).astype(BF16), (by_act * silu).astype(BF16)


def cuts(n):
    return [pl.ds(at, CHUNK) for at in range(0, n, CHUNK)]


def put_blocks(out, total):
    blocks, rows, _ = out.shape
    for p in range(blocks):
        out[p] = total[pl.ds(p * rows, rows), :].astype(BF16)


def whole(shape):
    return pl.BlockSpec(shape, lambda i: (0,) * len(shape), pipeline_mode=pl.Buffered(1))


def fixed(shape):
    return pl.BlockSpec(shape, lambda i: (0,) * len(shape))


def tile(rows, columns):
    return pl.BlockSpec((rows, columns), lambda i: (i, 0))


def tile_of_one(rows, columns):
    return pl.BlockSpec((None, rows, columns), lambda i: (0, i, 0))


def struct(shape, dtype=BF16):
    return jax.ShapeDtypeStruct(shape, dtype)


def solution(mesh):
    group = mesh.shape["dp"]
    side = math.isqrt(group)

    def gather_only(shards, layer):
        shapes = [w.shape[1:] for w in shards]

        def body(ins, outs, scratch):
            spot = Spot(side)
            greet_for_gather(spot)
            stages = [gather_stages(spot, ins[i], layer, outs[i], scratch[4 * i : 4 * i + 4]) for i in range(3)]
            for stage in zip(*stages, strict=True):
                for run in stage:
                    run()

        scratch = [one for shape in shapes for one in gather_scratch(*shape)]
        outs = [struct((group, *shape)) for shape in shapes]
        return call(body, 3, (), [ANY] * 3, [ANY] * 3, outs, scratch, 0, 1000)(*shards)

    def forward(x, weights, shards, layer):
        _, tokens, d = x.shape
        ff = weights[0].shape[1]
        steps = tokens // ROWS
        shapes = [w.shape[1:] for w in shards]

        def body(ins, outs, scratch):
            x, w_gate, w_up, w_down, *shards = ins
            a_out, gate_out, up_out, act_out, h_out, *full = outs
            i = pl.program_id(0)
            spot = Spot(side)
            stages = [gather_stages(spot, shards[j], layer, full[j], scratch[4 * j : 4 * j + 4]) for j in range(3)]
            for number, when in enumerate((0, 2, 4, 9, 12)):

                @pl.when(i == when)
                def _():
                    if number == 0:
                        greet_for_gather(spot)
                    for one in stages:
                        one[number]()

            wide = x[...].astype(F32)
            a = (wide * scale_of(wide)).astype(BF16)
            a_out[...] = a
            for cut in cuts(ff):
                gate, up = dot(a, w_gate[:, cut]), dot(a, w_up[:, cut])
                gate_out[:, cut], up_out[:, cut] = gate, up
                act_out[:, cut] = (gate * jax.nn.sigmoid(gate) * up).astype(BF16)
            h_out[...] = (wide + dot(act_out[...], w_down[...]).astype(BF16).astype(F32)).astype(BF16)

            @pl.when(i == steps - 1)
            def _():
                for one in stages:
                    one[5]()

        scratch = [one for shape in shapes for one in gather_scratch(*shape)]
        wide = [struct((tokens, ff), F32)] * 2
        outs = [struct((tokens, d)), *wide, struct((tokens, ff)), struct((tokens, d))] + [struct((group, *s)) for s in shapes]
        out_specs = [tile(ROWS, d)] + [tile(ROWS, ff)] * 3 + [tile(ROWS, d)] + [ANY] * 3
        in_specs = [tile_of_one(ROWS, d)] + [whole(w.shape) for w in weights] + [ANY] * 3
        return call(body, 7, (steps,), in_specs, out_specs, outs, scratch, 1, 6 * tokens * d * ff)(x, *weights, *shards)

    def last_layer(h, dy, weights):
        tokens, d = h.shape
        ff = weights[0].shape[1]
        steps = tokens // ROWS
        rows = ff // group

        def body(ins, outs, scratch):
            h, dy, w_gate, w_up, w_down = ins
            a_out, by_gate, by_up, by_h, by_down = outs
            total, act = scratch
            i = pl.program_id(0)

            @pl.when(i == 0)
            def _():
                total[...] = jnp.zeros_like(total)

            wide = h[...].astype(F32)
            scale = scale_of(wide)
            a = (wide * scale).astype(BF16)
            a_out[...] = a
            by_y = dy[...]
            for cut in cuts(ff):
                gate, up = dot(a, w_gate[:, cut]), dot(a, w_up[:, cut])
                by_act = dot_t(by_y, w_down[cut, :]).astype(BF16).astype(F32)
                silu, by_gate[:, cut], by_up[:, cut] = gated_back(gate, up, by_act)
                act[:, cut] = (silu * up).astype(BF16)
            by_a = dot_t(by_gate[...], w_gate[...]).astype(BF16).astype(F32) + dot_t(by_up[...], w_up[...]).astype(BF16).astype(F32)
            by_a = by_a.astype(BF16).astype(F32)
            inner = jnp.sum(by_a * wide, -1, keepdims=True) * (scale * scale * scale) * (1 / d)
            by_x = (by_a * scale - wide * inner).astype(BF16)
            by_h[...] = (by_y.astype(F32) + by_x.astype(F32)).astype(BF16)
            for cut in cuts(ff):
                total[cut, :] += dot(act[:, cut].T, by_y)

            @pl.when(i == steps - 1)
            def _():
                put_blocks(by_down, total)

        outs = [struct((tokens, d)), struct((tokens, ff)), struct((tokens, ff)), struct((tokens, d)), struct((group, rows, d))]
        out_specs = [tile(ROWS, d), tile(ROWS, ff), tile(ROWS, ff), tile(ROWS, d), fixed((group, rows, d))]
        in_specs = [tile(ROWS, d), tile_of_one(ROWS, d)] + [whole(w.shape) for w in weights]
        scratch = [pltpu.VMEM((ff, d), F32), pltpu.VMEM((ROWS, ff), BF16)]
        return call(body, 5, (steps,), in_specs, out_specs, outs, scratch, None, 12 * tokens * d * ff)(h, dy, *weights)

    def hidden(compute, n_in, n_out, n_scratch, firsts, seconds):
        more_in, more_specs, more_out, more_out_specs, more_scratch = [], [], [], [], []
        for _, blocks, shape in firsts:
            half = half_shape(*shape)
            if not isinstance(blocks, int):
                more_in += [blocks]
                more_specs += [ANY]
            more_out += [struct((side, 2, *half)), struct((2, *half), F32)]
            more_out_specs += [fixed((side, 2, *half)), fixed((2, *half))]
            more_scratch += ring_scratch(side, half)
        for _, (partial, kept) in seconds:
            half = partial.shape[2:]
            more_in += [partial, kept]
            more_specs += [ANY, whole(kept.shape)]
            more_out += [struct((2, *half))]
            more_out_specs += [fixed((2, *half))]
            more_scratch += ring_scratch(1, half)

        def body(ins, outs, scratch):
            i = pl.program_id(0)
            spot = Spot(side)
            ins_left, outs_left, rings = list(ins[n_in:]), list(outs[n_out:]), list(scratch[n_scratch:])
            plan = []
            for when, blocks, _ in firsts:
                source = scratch[blocks] if isinstance(blocks, int) else ins_left.pop(0)
                stages = first_ring(spot, source, rings[:13], outs_left.pop(0), outs_left.pop(0))
                del rings[:13]
                plan += list(zip(when, stages, strict=True))
            for when, _ in seconds:
                stages = second_ring(spot, ins_left.pop(0), ins_left.pop(0), rings[:13], outs_left.pop(0))
                del rings[:13]
                plan += list(zip(when, stages, strict=True))

            @pl.when(i == 0)
            def _():
                greet([spot.near(*way) for way in ((1, 0), (side - 1, 0), (0, 1), (0, side - 1))])

            for when, run in plan:
                if when >= 0:
                    pl.when(i == when)(run)
            compute(i, ins[:n_in], outs[:n_out], scratch[:n_scratch])
            for when, run in plan:
                if when < 0:
                    pl.when(i == pl.num_programs(0) + when)(run)

        return body, more_in, more_specs, more_out, more_out_specs, more_scratch

    def weight_gradient(a, by, number, firsts, seconds):
        tokens, m = a.shape
        n = by.shape[1]
        steps = tokens // TOKENS
        rows = m // group

        def compute(i, ins, outs, scratch):
            a, by = ins
            (total,) = scratch

            @pl.when(i == 0)
            def _():
                total[...] = jnp.zeros_like(total)

            right = by[...]
            for cut in cuts(m):
                total[cut, :] += dot(a[:, cut].T, right)

            @pl.when(i == steps - 1)
            def _():
                put_blocks(outs[0], total)

        body, ins, specs, outs, out_specs, scratch = hidden(compute, 2, 1, 1, firsts, seconds)
        return call(
            body,
            2 + len(ins),
            (steps,),
            [tile(TOKENS, m), tile(TOKENS, n), *specs],
            [fixed((group, rows, n)), *out_specs],
            [struct((group, rows, n)), *outs],
            [pltpu.VMEM((m, n), F32), *scratch],
            number,
            2 * tokens * m * n,
        )(a, by, *ins)

    def two_gradients(a, bys, width, number, firsts, seconds):
        tokens, m = a.shape
        steps = tokens // TOKENS
        rows = m // group

        def compute(i, ins, outs, scratch):
            a, *bys = ins
            total, blocks = scratch

            @pl.when(lax.rem(i, steps) == 0)
            def _():
                total[...] = jnp.zeros_like(total)

            def add(by):
                left = a[...].T
                for at in range(0, width, 256 if width % CHUNK else CHUNK):
                    cut = pl.ds(at, 256 if width % CHUNK else CHUNK)
                    total[:, cut] += dot(left, by[:, cut])

            if len(bys) == 1:
                add(bys[0])
            else:
                pl.when(i < steps)(lambda: add(bys[0]))
                pl.when(i >= steps)(lambda: add(bys[1]))
            pl.when(i == steps - 1)(lambda: put_blocks(blocks, total))
            pl.when(i == 2 * steps - 1)(lambda: put_blocks(outs[0], total))

        if len(bys) == 1:
            by_specs = [pl.BlockSpec((TOKENS, width), lambda i: (i % steps, i // steps))]
        else:
            by_specs = [
                pl.BlockSpec((TOKENS, width), lambda i: (jnp.minimum(i, steps - 1), 0)),
                pl.BlockSpec((TOKENS, width), lambda i: (jnp.maximum(i - steps, 0), 0)),
            ]
        n_in = 1 + len(bys)
        body, ins, specs, outs, out_specs, scratch = hidden(compute, n_in, 1, 2, firsts, seconds)
        return call(
            body,
            n_in + len(ins),
            (2 * steps,),
            [pl.BlockSpec((TOKENS, m), lambda i: (i % steps, 0)), *by_specs, *specs],
            [fixed((group, rows, width)), *out_specs],
            [struct((group, rows, width)), *outs],
            [pltpu.VMEM((m, width), F32), pltpu.VMEM((group, rows, width), BF16), *scratch],
            number,
            4 * tokens * m * width,
        )(a, *bys, *ins)

    def gate_gradient(by_h, gate, up, a, w_down, number, firsts, seconds):
        tokens, d = a.shape
        ff = gate.shape[1]
        steps = tokens // TOKENS
        rows = d // group

        def compute(i, ins, outs, scratch):
            by_h, gate, up, a, w_down = ins
            by_up, by_w = outs
            (total,) = scratch

            @pl.when(i == 0)
            def _():
                total[...] = jnp.zeros_like(total)

            by_y, left = by_h[...], a[...].T
            for cut in cuts(ff):
                by_act = dot_t(by_y, w_down[cut, :]).astype(BF16).astype(F32)
                _, by_gate, by_up[:, cut] = gated_back(gate[:, cut], up[:, cut], by_act)
                total[:, cut] += dot(left, by_gate)

            @pl.when(i == steps - 1)
            def _():
                put_blocks(by_w, total)

        body, ins, specs, outs, out_specs, scratch = hidden(compute, 5, 2, 1, firsts, seconds)
        return call(
            body,
            5 + len(ins),
            (steps,),
            [tile(TOKENS, d), tile(TOKENS, ff), tile(TOKENS, ff), tile(TOKENS, d), whole(w_down.shape), *specs],
            [tile(TOKENS, ff), fixed((group, rows, ff)), *out_specs],
            [struct((tokens, ff)), struct((group, rows, ff)), *outs],
            [pltpu.VMEM((d, ff), F32), *scratch],
            number,
            4 * tokens * d * ff,
        )(by_h, gate, up, a, w_down, *ins)

    def closing(first, seconds, ready, number):
        half = half_shape(*first.shape[1:])
        n, m = len(ready), len(seconds)

        def body(ins, outs, scratch):
            blocks, *rest = ins
            *late, last, squares = outs
            spot = Spot(side)
            others = [(df, ds) for df in range(side) for ds in range(side) if df or ds]
            greet([spot.near(*way) for way in others])
            rings = [scratch[13 * at : 13 * at + 13] for at in range(m + 2)]
            partial, kept, sums, out, came = scratch[13 * (m + 2) :]
            one = first_ring(spot, blocks, rings[0], partial, kept)
            seconds = [second_ring(spot, rest[2 * at], rest[2 * at + 1], rings[1 + at], late[at]) for at in range(m)]
            final = second_ring(spot, partial, kept, rings[m + 1], last)
            one[0]()
            for second in seconds:
                second[0]()
            for second in seconds:
                second[1]()
            one[1]()
            for second in seconds:
                second[2]()
            total = jnp.zeros((1, 1), F32)

            def added(total, g):
                for h in range(2):
                    wide = g[h].astype(F32)
                    total = total + jnp.sum(wide * wide, keepdims=True)
                return total

            for g in [*rest[2 * m :], *late]:
                total = added(total, g)
            one[2]()
            for run in final:
                run()
            total = added(total, last)
            sums[0] = jnp.broadcast_to(total, sums.shape[1:])
            for at, way in enumerate(others):
                send(sums.at[0], sums.at[1 + at], out.at[at], came.at[at], dp=spot.near(*way))
            for at in range(len(others)):
                await_bytes(sums.at[0], came.at[at])
                total = total + sums[1 + at, 0:1, 0:1]
            squares[...] = jnp.broadcast_to(total, squares.shape)
            for at in range(len(others)):
                await_bytes(sums.at[0], out.at[at])

        vmem = pl.BlockSpec(memory_space=pltpu.VMEM)
        scratch = ring_scratch(side, half)
        for partial, _ in seconds:
            scratch += ring_scratch(1, partial.shape[2:])
        scratch += ring_scratch(1, half)
        scratch += [pltpu.VMEM((side, 2, *half), BF16), pltpu.VMEM((2, *half), F32), pltpu.VMEM((group, 8, 128), F32)]
        scratch += [DMA((group - 1,)), DMA((group - 1,))]
        outs = [struct((2, *partial.shape[2:])) for partial, _ in seconds] + [struct((2, *half)), struct((8, 128), F32)]
        in_specs = [ANY] + [ANY, vmem] * m + [vmem] * n
        return call(body, 1 + 2 * m + n, (), in_specs, [vmem] * len(outs), outs, scratch, number, 1000)(
            first, *[one for second in seconds for one in second], *ready
        )

    def adamw(w, m, v, g):
        m = 0.9 * m + 0.1 * g
        v = 0.95 * v + 0.05 * g * g
        step = m * lax.rsqrt(v + 1e-8) + 0.1 * w
        return (w - 0.02 * step).astype(BF16), m, v

    def joined(g, shape):
        return jnp.concatenate(list(g), 1 if shape[1] > 1024 else 0)

    def step(x, dy, *arrays):
        weights, m, v = (arrays[i : i + 3] for i in (0, 3, 6))
        d, ff = weights[2].shape[2], weights[0].shape[2]
        flat = lambda full: [w.reshape(-1, w.shape[2]) for w in full]
        w_0 = flat(gather_only(weights, 0))
        a_0, gate, up, act, h, *full = forward(x, w_0, weights, 1)
        a_1, by_gate, by_up, by_h, down_1 = last_layer(h, dy, flat(full))
        shape, cut = (d // group, ff), (d // group, ff // 2)
        down_shape = (ff // group, d)
        up_1, *rings = two_gradients(
            a_1, (by_gate, by_up), ff, 2, [((0, 5, 10), down_1, down_shape), ((8, 13, -1), 1, shape)], []
        )
        down_1, gate_1 = rings[:2], rings[2:]
        down_0, *up_1, down_1, gate_1 = weight_gradient(
            act, by_h, 3, [((0, 5, -1), up_1, shape)], [((0, 3, 6), down_1), ((1, 4, 7), gate_1)]
        )
        by_up, gate_0, *down_0, up_1 = gate_gradient(
            by_h, gate, up, a_0, w_0[2], 4, [((0, 3, 5), down_0, down_shape)], [((0, 2, 4), up_1)]
        )
        up_0b, *rings, down_0 = two_gradients(
            a_0, (by_up,), ff // 2, 5, [((0, 9, 13), gate_0, shape), ((9, 13, -1), 1, cut)], [((0, 4, 8), down_0)]
        )
        gate_0, up_0a, up_0b, squares = closing(up_0b, [rings[:2], rings[2:]], [down_1, gate_1, up_1, down_0], 6)
        up_0 = jnp.concatenate([up_0a, up_0b], 0)
        count = group * sum(w.size for w in weights)
        factor = jnp.minimum(1.0, 0.5 * lax.rsqrt(squares[0, 0] / count + 1e-30))
        pairs = ((gate_0, gate_1), (up_0, up_1), (down_0, down_1))
        new = []
        for w, m_w, v_w, pair in zip(weights, m, v, pairs, strict=True):
            g = jnp.stack([joined(one, w.shape[1:]) for one in pair]).astype(F32) * factor
            new.append(adamw(w.astype(F32), m_w, v_w, g))
        return tuple(one[which] for which in range(3) for one in new)

    states, cut = P(("rep", "dp"), None, None), P(None, "dp", None)
    return jax.shard_map(
        step,
        mesh=mesh,
        in_specs=(states, states) + (cut,) * 9,
        out_specs=(P("rep", "dp", None),) * 9,
        check_vma=False,
    )
```

```python
import math

import jax
import jax.numpy as jnp
from jax import lax
from jax.experimental import pallas as pl
from jax.experimental.pallas import tpu as pltpu
from jax.sharding import PartitionSpec as P

MESH = pl.DeviceIdType.MESH
F32, BF16 = jnp.float32, jnp.bfloat16
ANY = pl.BlockSpec(memory_space=pl.ANY)
DMA = pltpu.SemaphoreType.DMA
CHUNK, FINE, COARSE = 512, 256, 1280
ROWS, TOKENS = 512, 512


class Spot:
    def __init__(self, side):
        self.side = side
        rep, self.dp = lax.axis_index("rep"), lax.axis_index("dp")
        c = self.c = lax.rem(rep, 2)
        hi, lo = self.dp // side, lax.rem(self.dp, side)
        self.f, self.s = hi * c + lo * (1 - c), lo * c + hi * (1 - c)
        self.partner = rep + 1 - 2 * c

    def at(self, f, s):
        f, s, c, side = lax.rem(f, self.side), lax.rem(s, self.side), self.c, self.side
        return f * (1 - c + side * c) + s * (side * (1 - c) + c)

    def near(self, df, ds):
        return self.at(self.f + df, self.s + ds)


def greet(places, partner=None):
    barrier = pltpu.get_barrier_semaphore()
    for place in places:
        pl.semaphore_signal(barrier, inc=1, device_id={"dp": place}, device_id_type=MESH)
    if partner is not None:
        pl.semaphore_signal(barrier, inc=1, device_id={"rep": partner}, device_id_type=MESH)
    pl.semaphore_wait(barrier, len(places) + (partner is not None))


def send(src, dst, out, came, **to):
    pltpu.make_async_remote_copy(src_ref=src, dst_ref=dst, send_sem=out, recv_sem=came, device_id=to, device_id_type=MESH).start()


def bring(src, dst, sem):
    pltpu.make_async_copy(src, dst, sem).start()


def await_bytes(like, sem):
    pltpu.make_async_copy(like, like, sem).wait()


def call(body, n, grid, in_specs, out_specs, out_shape, scratch, number, cost):
    def kernel(*refs):
        body(refs[:n], refs[n : n + len(out_shape)], refs[n + len(out_shape) :])

    return pl.pallas_call(
        kernel,
        grid=grid,
        in_specs=in_specs,
        out_specs=out_specs,
        out_shape=out_shape,
        scratch_shapes=scratch,
        compiler_params=pltpu.CompilerParams(
            dimension_semantics=("arbitrary",) * len(grid),
            vmem_limit_bytes=66_000_000,
            **({} if number is None else {"collective_id": number, "has_side_effects": True}),
        ),
        cost_estimate=pl.CostEstimate(flops=cost, bytes_accessed=cost // 400, transcendentals=0),
    )


def gather_scratch(rows, columns):
    return [pltpu.VMEM((rows, columns), BF16), DMA((2,)), DMA((2,)), DMA((9,))]


def gather_stages(spot, shards, layer, full, scratch):
    held, local, out, came = scratch
    rows, columns = held.shape
    by_columns = columns > 1024
    side = spot.side
    me, c = spot.dp, spot.c

    def part(ref, lead, cuts, number):
        if by_columns:
            width = columns // cuts
            return ref.at[lead, :, pl.ds(pl.multiple_of(number * width, 128), width)]
        height = rows // cuts
        return ref.at[lead, pl.ds(pl.multiple_of(number * height, 8), height), :]

    def unit(p):
        return part(full, p, 2, c)

    def quarter(p, q):
        return part(full, p, 4, 2 * c + q)

    def units(n):
        return part(full, pl.ds(0, n), 2, 0)

    def quarters(n):
        return part(full, pl.ds(0, n), 4, 0)

    mine = part(shards, layer, 2, c)

    def start():
        send(mine, unit(me), out.at[0], came.at[0], dp=spot.near(1, 0))
        send(mine, unit(me), out.at[0], came.at[6], dp=spot.near(side - 1, 0))
        fill = pltpu.make_async_copy(shards.at[layer], held, local.at[0])
        fill.start()
        fill.wait()
        bring(held, full.at[me], local.at[1])

    def relay():
        p, q = spot.near(side - 1, 0), spot.near(1, 0)
        await_bytes(unit(p), came.at[0])
        send(quarter(p, 0), quarter(p, 0), out.at[0], came.at[7], dp=spot.near(1, 0))
        await_bytes(unit(q), came.at[6])
        send(quarter(q, 1), quarter(q, 1), out.at[0], came.at[8], dp=spot.near(side - 1, 0))

    def across():
        await_bytes(quarter(me, 0), came.at[7])
        await_bytes(quarter(me, 1), came.at[8])
        for df in range(side):
            p = spot.near(df, 0)
            source = unit(p) if df else mine
            send(source, unit(p), out.at[0], came.at[1], dp=spot.near(0, 1))
            send(source, unit(p), out.at[0], came.at[2], dp=spot.near(0, side - 1))
            if df:
                send(unit(p), unit(p), out.at[1], came.at[5], rep=spot.partner)

    def onward():
        await_bytes(units(side), came.at[1])
        await_bytes(units(side), came.at[2])
        for df in range(side):
            p, q = spot.near(df, side - 1), spot.near(df, 1)
            send(quarter(p, 0), quarter(p, 0), out.at[0], came.at[3], dp=spot.near(0, 1))
            send(quarter(q, 1), quarter(q, 1), out.at[0], came.at[4], dp=spot.near(0, side - 1))
        for df in range(side):
            for ds in (1, side - 1):
                p = spot.near(df, ds)
                send(unit(p), unit(p), out.at[1], came.at[5], rep=spot.partner)

    def last():
        await_bytes(quarters(side), came.at[3])
        await_bytes(quarters(side), came.at[4])
        for df in range(side):
            p = spot.near(df, 2)
            send(unit(p), unit(p), out.at[1], came.at[5], rep=spot.partner)

    def finish():
        n = side * side - 1
        await_bytes(units(n), came.at[5])
        await_bytes(units(n), out.at[0])
        await_bytes(units(n), out.at[1])
        await_bytes(held, local.at[1])

    return start, relay, across, onward, last, finish


def greet_for_gather(spot):
    greet([spot.near(df, ds) for df, ds in ((1, 0), (spot.side - 1, 0), (0, 1), (0, spot.side - 1))], spot.partner)


def half_shape(rows, columns):
    return (rows, columns // 2) if columns > 1024 else (rows // 2, columns)


def half_of(ref, p, h):
    rows, columns = ref.shape[1:]
    if columns > 1024:
        return ref.at[p, :, pl.ds(h * (columns // 2), columns // 2)]
    return ref.at[p, pl.ds(h * (rows // 2), rows // 2), :]


def ring_scratch(n, half):
    here = (n, *half) if n > 1 else (1, 16, 128)
    return [pltpu.VMEM((n, *half), BF16)] * 4 + [pltpu.VMEM(here, BF16)] * 2 + [pltpu.VMEM((n, *half), BF16)] * 4 + [DMA((4,)), DMA((6,)), DMA((6,))]


def ring_stages(source, place, side, plus, minus, scratch, own, done):
    across_a, across_b, next_a, prev_b, here_a, here_b, up_a, up_b, down_a, down_b, local, out, came = scratch
    n = across_a.shape[0]
    following, before, opposite = (lax.rem(place + d, side) for d in (1, side - 1, 2))

    def start():
        for k in range(n):
            send(source(opposite, k, 0), across_a.at[k], out.at[0], came.at[0], dp=plus)
            send(source(opposite, k, 1), across_b.at[k], out.at[1], came.at[1], dp=minus)
        for k in range(n):
            send(source(following, k, 1), up_b.at[k], out.at[2], came.at[2], dp=plus)
            send(source(before, k, 0), down_a.at[k], out.at[3], came.at[3], dp=minus)
        for k in range(n):
            bring(source(following, k, 0), next_a.at[k], local.at[0])
            bring(source(before, k, 1), prev_b.at[k], local.at[1])
            if own is None:
                bring(source(place, k, 0), here_a.at[k], local.at[2])
                bring(source(place, k, 1), here_b.at[k], local.at[3])

    def add():
        for which, (mine, theirs, landing, to) in enumerate(((next_a, across_a, up_a, plus), (prev_b, across_b, down_b, minus))):
            await_bytes(mine, local.at[which])
            await_bytes(theirs, came.at[which])
            for k in range(n):
                mine[k] = (mine[k].astype(F32) + theirs[k].astype(F32)).astype(BF16)
            for k in range(n):
                send(mine.at[k], landing.at[k], out.at[4 + which], came.at[4 + which], dp=to)

    def finish():
        if own is None:
            await_bytes(here_a, local.at[2])
            await_bytes(here_b, local.at[3])
        for number, ref in zip((2, 3, 4, 5), (up_b, down_a, up_a, down_b), strict=True):
            await_bytes(ref, came.at[number])
        for k in range(n):
            for h, here, up, down in ((0, here_a, up_a, down_a), (1, here_b, up_b, down_b)):
                term = here[k].astype(F32) if own is None else own[h]
                done(k, h, term + up[k].astype(F32) + down[k].astype(F32))
        for number in range(6):
            await_bytes(across_a, out.at[number])

    return start, add, finish


def first_ring(spot, blocks, scratch, partial, kept):
    def done(k, h, total):
        partial[k, h] = total.astype(BF16)

        @pl.when(spot.s == k)
        def _():
            kept[h] = total

    def source(j, k, h):
        return half_of(blocks, spot.at(j, k), h)

    return ring_stages(source, spot.f, spot.side, spot.near(1, 0), spot.near(spot.side - 1, 0), scratch, None, done)


def second_ring(spot, partial, kept, scratch, result):
    def done(k, h, total):
        result[h] = total.astype(BF16)

    def source(j, k, h):
        return partial.at[j, h]

    return ring_stages(source, spot.s, spot.side, spot.near(0, 1), spot.near(0, spot.side - 1), scratch, kept, done)


def dot(a, b):
    return jnp.dot(a, b, preferred_element_type=F32)


def dot_t(a, b):
    return lax.dot_general(a, b, (((1,), (1,)), ((), ())), preferred_element_type=F32)


def scale_of(wide):
    return lax.rsqrt(jnp.mean(wide * wide, -1, keepdims=True) + 1e-6)


def gated_back(gate, up, by_act):
    s = jax.nn.sigmoid(gate)
    silu = gate * s
    return silu, (by_act * up * (s + silu * (1 - s))).astype(BF16), (by_act * silu).astype(BF16)


def cuts(n, width=CHUNK):
    return [pl.ds(at, width) for at in range(0, n, width)]


def put_blocks(out, total):
    blocks, rows, _ = out.shape
    for p in range(blocks):
        out[p] = total[pl.ds(p * rows, rows), :].astype(BF16)


def whole(shape):
    return pl.BlockSpec(shape, lambda i: (0,) * len(shape), pipeline_mode=pl.Buffered(1))


def fixed(shape):
    return pl.BlockSpec(shape, lambda i: (0,) * len(shape))


def tile(rows, columns):
    return pl.BlockSpec((rows, columns), lambda i: (i, 0))


def tile_of_one(rows, columns):
    return pl.BlockSpec((None, rows, columns), lambda i: (0, i, 0))


def struct(shape, dtype=BF16):
    return jax.ShapeDtypeStruct(shape, dtype)


def solution(mesh):
    group = mesh.shape["dp"]
    side = math.isqrt(group)

    def gather_only(shards, layer):
        shapes = [w.shape[1:] for w in shards]

        def body(ins, outs, scratch):
            spot = Spot(side)
            greet_for_gather(spot)
            stages = [gather_stages(spot, ins[i], layer, outs[i], scratch[4 * i : 4 * i + 4]) for i in range(3)]
            for stage in zip(*stages, strict=True):
                for run in stage:
                    run()

        scratch = [one for shape in shapes for one in gather_scratch(*shape)]
        outs = [struct((group, *shape)) for shape in shapes]
        return call(body, 3, (), [ANY] * 3, [ANY] * 3, outs, scratch, 0, 1000)(*shards)

    def forward(x, weights, shards, layer):
        _, tokens, d = x.shape
        ff = weights[0].shape[1]
        steps = tokens // ROWS
        shapes = [w.shape[1:] for w in shards]

        def body(ins, outs, scratch):
            x, w_gate, w_up, w_down, *shards = ins
            a_out, gate_out, up_out, act_out, h_out, *full = outs
            i = pl.program_id(0)
            spot = Spot(side)
            stages = [gather_stages(spot, shards[j], layer, full[j], scratch[4 * j : 4 * j + 4]) for j in range(3)]
            for number, when in enumerate((0, 1, 2, 5, 6)):

                @pl.when(i == when)
                def _():
                    if number == 0:
                        greet_for_gather(spot)
                    for one in stages:
                        one[number]()

            wide = x[...].astype(F32)
            a = (wide * scale_of(wide)).astype(BF16)
            a_out[...] = a
            for cut in cuts(ff):
                gate, up = dot(a, w_gate[:, cut]), dot(a, w_up[:, cut])
                gate_out[:, cut], up_out[:, cut] = gate, up
                act_out[:, cut] = (gate * jax.nn.sigmoid(gate) * up).astype(BF16)
            h_out[...] = (wide + dot(act_out[...], w_down[...]).astype(BF16).astype(F32)).astype(BF16)

            @pl.when(i == steps - 1)
            def _():
                for one in stages:
                    one[5]()

        scratch = [one for shape in shapes for one in gather_scratch(*shape)]
        wide = [struct((tokens, ff), F32)] * 2
        outs = [struct((tokens, d)), *wide, struct((tokens, ff)), struct((tokens, d))] + [struct((group, *s)) for s in shapes]
        out_specs = [tile(ROWS, d)] + [tile(ROWS, ff)] * 3 + [tile(ROWS, d)] + [ANY] * 3
        in_specs = [tile_of_one(ROWS, d)] + [whole(w.shape) for w in weights] + [ANY] * 3
        return call(body, 7, (steps,), in_specs, out_specs, outs, scratch, 1, 6 * tokens * d * ff)(x, *weights, *shards)

    def last_layer(h, dy, weights):
        tokens, d = h.shape
        ff = weights[0].shape[1]
        steps = tokens // ROWS
        rows = ff // group

        def body(ins, outs, scratch):
            h, dy, w_gate, w_up, w_down = ins
            a_out, by_gate, by_up, by_h, by_down = outs
            total, act = scratch
            i = pl.program_id(0)

            @pl.when(i == 0)
            def _():
                total[...] = jnp.zeros_like(total)

            wide = h[...].astype(F32)
            scale = scale_of(wide)
            a = (wide * scale).astype(BF16)
            a_out[...] = a
            by_y = dy[...]
            for cut in cuts(ff, FINE):
                gate, up = dot(a, w_gate[:, cut]), dot(a, w_up[:, cut])
                by_act = dot_t(by_y, w_down[cut, :]).astype(BF16).astype(F32)
                silu, by_gate[:, cut], by_up[:, cut] = gated_back(gate, up, by_act)
                act[:, cut] = (silu * up).astype(BF16)
            by_a = dot_t(by_gate[...], w_gate[...]).astype(BF16).astype(F32) + dot_t(by_up[...], w_up[...]).astype(BF16).astype(F32)
            by_a = by_a.astype(BF16).astype(F32)
            inner = jnp.sum(by_a * wide, -1, keepdims=True) * (scale * scale * scale) * (1 / d)
            by_x = (by_a * scale - wide * inner).astype(BF16)
            by_h[...] = (by_y.astype(F32) + by_x.astype(F32)).astype(BF16)
            for cut in cuts(ff, FINE):
                total[cut, :] += dot(act[:, cut].T, by_y)

            @pl.when(i == steps - 1)
            def _():
                put_blocks(by_down, total)

        outs = [struct((tokens, d)), struct((tokens, ff)), struct((tokens, ff)), struct((tokens, d)), struct((group, rows, d))]
        out_specs = [tile(ROWS, d), tile(ROWS, ff), tile(ROWS, ff), tile(ROWS, d), fixed((group, rows, d))]
        in_specs = [tile(ROWS, d), tile_of_one(ROWS, d)] + [whole(w.shape) for w in weights]
        scratch = [pltpu.VMEM((ff, d), F32), pltpu.VMEM((ROWS, ff), BF16)]
        return call(body, 5, (steps,), in_specs, out_specs, outs, scratch, None, 12 * tokens * d * ff)(h, dy, *weights)

    def hidden(compute, n_in, n_out, n_scratch, firsts, seconds):
        more_in, more_specs, more_out, more_out_specs, more_scratch = [], [], [], [], []
        for _, blocks, shape in firsts:
            half = half_shape(*shape)
            if not isinstance(blocks, int):
                more_in += [blocks]
                more_specs += [ANY]
            more_out += [struct((side, 2, *half)), struct((2, *half), F32)]
            more_out_specs += [fixed((side, 2, *half)), fixed((2, *half))]
            more_scratch += ring_scratch(side, half)
        for _, second in seconds:
            if isinstance(second, int):
                half = half_shape(*firsts[second][2])
            else:
                partial, kept = second
                half = partial.shape[2:]
                more_in += [partial, kept]
                more_specs += [ANY, whole(kept.shape)]
            more_out += [struct((2, *half))]
            more_out_specs += [fixed((2, *half))]
            more_scratch += ring_scratch(1, half)

        def body(ins, outs, scratch):
            i = pl.program_id(0)
            spot = Spot(side)
            ins_left, outs_left, rings = list(ins[n_in:]), list(outs[n_out:]), list(scratch[n_scratch:])
            plan = []
            partials = []
            for when, blocks, _ in firsts:
                source = scratch[blocks] if isinstance(blocks, int) else ins_left.pop(0)
                partials.append((outs_left.pop(0), outs_left.pop(0)))
                stages = first_ring(spot, source, rings[:13], *partials[-1])
                del rings[:13]
                plan += list(zip(when, stages, strict=True))
            for when, second in seconds:
                partial, kept = partials[second] if isinstance(second, int) else (ins_left.pop(0), ins_left.pop(0))
                stages = second_ring(spot, partial, kept, rings[:13], outs_left.pop(0))
                del rings[:13]
                plan += list(zip(when, stages, strict=True))

            @pl.when(i == 0)
            def _():
                greet([spot.near(*way) for way in ((1, 0), (side - 1, 0), (0, 1), (0, side - 1))])

            for when, run in plan:
                if when >= 0:
                    pl.when(i == when)(run)
            compute(i, ins[:n_in], outs[:n_out], scratch[:n_scratch])
            for when, run in plan:
                if when < 0:
                    pl.when(i == pl.num_programs(0) + when)(run)

        return body, more_in, more_specs, more_out, more_out_specs, more_scratch

    def weight_gradient(a, by, number, firsts, seconds):
        tokens, m = a.shape
        n = by.shape[1]
        steps = tokens // TOKENS
        rows = m // group

        def compute(i, ins, outs, scratch):
            a, by = ins
            (total,) = scratch

            @pl.when(i == 0)
            def _():
                total[...] = jnp.zeros_like(total)

            right = by[...]
            for cut in cuts(m):
                total[cut, :] += dot(a[:, cut].T, right)

            @pl.when(i == steps - 1)
            def _():
                put_blocks(outs[0], total)

        body, ins, specs, outs, out_specs, scratch = hidden(compute, 2, 1, 1, firsts, seconds)
        return call(
            body,
            2 + len(ins),
            (steps,),
            [tile(TOKENS, m), tile(TOKENS, n), *specs],
            [fixed((group, rows, n)), *out_specs],
            [struct((group, rows, n)), *outs],
            [pltpu.VMEM((m, n), F32), *scratch],
            number,
            2 * tokens * m * n,
        )(a, by, *ins)

    def two_gradients(a, bys, width, number, firsts, seconds):
        tokens, m = a.shape
        steps = tokens // TOKENS
        rows = m // group

        def compute(i, ins, outs, scratch):
            a, *bys = ins
            total, blocks = scratch

            @pl.when(lax.rem(i, steps) == 0)
            def _():
                total[...] = jnp.zeros_like(total)

            def add(by):
                left = a[...].T
                for cut in cuts(width, FINE if width % CHUNK else CHUNK):
                    total[:, cut] += dot(left, by[:, cut])

            if len(bys) == 1:
                add(bys[0])
            else:
                pl.when(i < steps)(lambda: add(bys[0]))
                pl.when(i >= steps)(lambda: add(bys[1]))
            pl.when(i == steps - 1)(lambda: put_blocks(blocks, total))
            pl.when(i == 2 * steps - 1)(lambda: put_blocks(outs[0], total))

        if len(bys) == 1:
            by_specs = [pl.BlockSpec((TOKENS, width), lambda i: (i % steps, i // steps))]
        else:
            by_specs = [
                pl.BlockSpec((TOKENS, width), lambda i: (jnp.minimum(i, steps - 1), 0)),
                pl.BlockSpec((TOKENS, width), lambda i: (jnp.maximum(i - steps, 0), 0)),
            ]
        n_in = 1 + len(bys)
        body, ins, specs, outs, out_specs, scratch = hidden(compute, n_in, 1, 2, firsts, seconds)
        return call(
            body,
            n_in + len(ins),
            (2 * steps,),
            [pl.BlockSpec((TOKENS, m), lambda i: (i % steps, 0)), *by_specs, *specs],
            [fixed((group, rows, width)), *out_specs],
            [struct((group, rows, width)), *outs],
            [pltpu.VMEM((m, width), F32), pltpu.VMEM((group, rows, width), BF16), *scratch],
            number,
            4 * tokens * m * width,
        )(a, *bys, *ins)

    def gate_gradient(by_h, gate, up, a, w_down, number, firsts, seconds):
        tokens, d = a.shape
        ff = gate.shape[1]
        steps = tokens // TOKENS
        rows = d // group

        def compute(i, ins, outs, scratch):
            by_h, gate, up, a, w_down = ins
            by_up, by_w = outs
            (total,) = scratch

            @pl.when(i == 0)
            def _():
                total[...] = jnp.zeros_like(total)

            by_y, left = by_h[...], a[...].T
            for cut in cuts(ff, COARSE):
                by_act = dot_t(by_y, w_down[cut, :]).astype(BF16).astype(F32)
                _, by_gate, by_up[:, cut] = gated_back(gate[:, cut], up[:, cut], by_act)
                total[:, cut] += dot(left, by_gate)

            @pl.when(i == steps - 1)
            def _():
                put_blocks(by_w, total)

        body, ins, specs, outs, out_specs, scratch = hidden(compute, 5, 2, 1, firsts, seconds)
        return call(
            body,
            5 + len(ins),
            (steps,),
            [tile(TOKENS, d), tile(TOKENS, ff), tile(TOKENS, ff), tile(TOKENS, d), whole(w_down.shape), *specs],
            [tile(TOKENS, ff), fixed((group, rows, ff)), *out_specs],
            [struct((tokens, ff)), struct((group, rows, ff)), *outs],
            [pltpu.VMEM((d, ff), F32), *scratch],
            number,
            4 * tokens * d * ff,
        )(by_h, gate, up, a, w_down, *ins)

    def closing(first, seconds, ready, count, number):
        half = half_shape(*first.shape[1:])
        n, m = len(ready), len(seconds)

        def body(ins, outs, scratch):
            blocks, *rest = ins
            *late, last, factor = outs
            spot = Spot(side)
            others = [(df, ds) for df in range(side) for ds in range(side) if df or ds]
            greet([spot.near(*way) for way in others])
            rings = [scratch[13 * at : 13 * at + 13] for at in range(m + 2)]
            partial, kept, sums, out, came = scratch[13 * (m + 2) :]
            one = first_ring(spot, blocks, rings[0], partial, kept)
            seconds = [second_ring(spot, rest[2 * at], rest[2 * at + 1], rings[1 + at], late[at]) for at in range(m)]
            final = second_ring(spot, partial, kept, rings[m + 1], last)
            one[0]()
            for second in seconds:
                second[0]()
            for second in seconds:
                second[1]()
            one[1]()
            for second in seconds:
                second[2]()
            total = jnp.zeros((1, 1), F32)

            def added(total, g):
                for h in range(2):
                    wide = g[h].astype(F32)
                    total = total + jnp.sum(wide * wide, keepdims=True)
                return total

            for g in [*rest[2 * m :], *late]:
                total = added(total, g)
            one[2]()
            for run in final:
                run()
            total = added(total, last)
            sums[0] = jnp.broadcast_to(total, sums.shape[1:])
            for at, way in enumerate(others):
                send(sums.at[0], sums.at[1 + at], out.at[at], came.at[at], dp=spot.near(*way))
            for at in range(len(others)):
                await_bytes(sums.at[0], came.at[at])
                total = total + sums[1 + at, 0:1, 0:1]
            factor[...] = jnp.minimum(1.0, 0.5 * lax.rsqrt(total / count + 1e-30))
            for at in range(len(others)):
                await_bytes(sums.at[0], out.at[at])

        vmem = pl.BlockSpec(memory_space=pltpu.VMEM)
        scratch = ring_scratch(side, half)
        for partial, _ in seconds:
            scratch += ring_scratch(1, partial.shape[2:])
        scratch += ring_scratch(1, half)
        scratch += [pltpu.VMEM((side, 2, *half), BF16), pltpu.VMEM((2, *half), F32), pltpu.VMEM((group, 8, 128), F32)]
        scratch += [DMA((group - 1,)), DMA((group - 1,))]
        outs = [struct((2, *partial.shape[2:])) for partial, _ in seconds] + [struct((2, *half)), struct((1, 1), F32)]
        in_specs = [ANY] + [ANY, vmem] * m + [vmem] * n
        return call(body, 1 + 2 * m + n, (), in_specs, [vmem] * len(outs), outs, scratch, number, 1000)(
            first, *[one for second in seconds for one in second], *ready
        )

    def adamw(w, m, v, g):
        m = 0.9 * m + 0.1 * g
        v = 0.95 * v + 0.05 * g * g
        step = m * lax.rsqrt(v + 1e-8) + 0.1 * w
        return (w - 0.02 * step).astype(BF16), m, v

    def joined(g, shape):
        return jnp.concatenate(list(g), 1 if shape[1] > 1024 else 0)

    def step(x, dy, *arrays):
        weights, m, v = (arrays[i : i + 3] for i in (0, 3, 6))
        d, ff = weights[2].shape[2], weights[0].shape[2]
        flat = lambda full: [w.reshape(-1, w.shape[2]) for w in full]
        w_0 = flat(gather_only(weights, 0))
        a_0, gate, up, act, h, *full = forward(x, w_0, weights, 1)
        a_1, by_gate, by_up, by_h, down_1 = last_layer(h, dy, flat(full))
        shape, cut = (d // group, ff), (d // group, ff // 2)
        down_shape = (ff // group, d)
        up_1, *rings = two_gradients(
            a_1, (by_gate, by_up), ff, 2, [((0, 5, 9), down_1, down_shape), ((8, 13, -1), 1, shape)], []
        )
        down_1, gate_1 = rings[:2], rings[2:]
        down_0, *up_1, down_1 = weight_gradient(act, by_h, 3, [((0, 5, -1), up_1, shape)], [((0, 3, 5), down_1)])
        by_up, gate_0, _, _, gate_1, up_1, down_0 = gate_gradient(
            by_h, gate, up, a_0, w_0[2], 4,
            [((0, 2, 3), down_0, down_shape)],
            [((0, 1, 2), gate_1), ((0, 1, 3), up_1), ((3, 4, 6), 0)],
        )
        up_0b, *rings = two_gradients(a_0, (by_up,), ff // 2, 5, [((0, 9, 13), gate_0, shape), ((8, 13, -1), 1, cut)], [])
        count = group * sum(w.size for w in weights)
        gate_0, up_0a, up_0b, factor = closing(up_0b, [rings[:2], rings[2:]], [down_1, gate_1, up_1, down_0], count, 6)
        up_0 = jnp.concatenate([up_0a, up_0b], 0)
        pairs = ((gate_0, gate_1), (up_0, up_1), (down_0, down_1))
        new = []
        for w, m_w, v_w, pair in zip(weights, m, v, pairs, strict=True):
            g = jnp.stack([joined(one, w.shape[1:]) for one in pair]).astype(F32) * factor
            new.append(adamw(w.astype(F32), m_w, v_w, g))
        return tuple(one[which] for which in range(3) for one in new)

    states, cut = P(("rep", "dp"), None, None), P(None, "dp", None)
    return jax.shard_map(
        step,
        mesh=mesh,
        in_specs=(states, states) + (cut,) * 9,
        out_specs=(P("rep", "dp", None),) * 9,
        check_vma=False,
    )
```
